32 devices in a mesh: area: 4 (over z), rank: 8 (over y, x, core).
Axes of the slice: x: 2, y: 2, z: 4, core: 2. Of those that a mesh axis runs over, the one named last changes fastest.
Arguments:
- membrane: float32 [4, 32768], P(None, ('area', 'rank')), may hold values from -6 to 6
- synaptic_trace: float32 [4, 32768], P(None, ('area', 'rank')), may hold values from 0 to 2
- pending: float32 [2, 4, 32768], P(None, None, ('area', 'rank')), may hold values from -6 to 6
- inter_input: float32 [10, 4, 32768], P(None, None, ('area', 'rank')), may hold values from -4 to 4
- ext_spikes: int32 [10, 4, 32768], P(None, None, ('area', 'rank')), may hold values from 0 to 3
- mem_decay: float32 [32768], P(('area', 'rank')), may hold values from 0.6 to 0.95
- trace_decay_factor: float32 [32768], P(('area', 'rank')), may hold values from 0.3 to 0.8
- threshold: float32 [32768], P(('area', 'rank')), may hold values from 0.5 to 1.5
- weight_tiles: bfloat16 [4, 8, 2, 1024, 1024], P('area', 'rank'), may hold values from -0.125 to 0.125
- tile_source: int32 [4, 8, 2], P('area', 'rank'), may hold values from 0 to 7, as said below
- send_amp: bfloat16 [4, 8, 4, 4, 128], P('area', 'rank'), may hold values from -6 to 6
- send_target: int32 [4, 8, 4, 4, 128], P('area', 'rank'), may hold values from 0 to 10239
- send_count: int32 [4, 8, 4, 4], P('area', 'rank'), may hold values from 0 to 128, as said below
Outputs:
- voltage_final: float32 [4, 32768], P(None, ('area', 'rank'))
- trace_final: float32 [4, 32768], P(None, ('area', 'rank'))
- late_traces: bfloat16 [2, 4, 32768], P(None, None, ('area', 'rank'))
- delivered: float32 [10, 4, 32768], P(None, None, ('area', 'rank'))
The draws below stay inside these ranges and needn't reach their ends.
Inputs may be any that keep to these rules, and one draw needn't show every extreme that they name: For each area a and each k, tile_source[a, :, k] is a permutation of 0 to 7. Entries of a list from slot send_count on are padding.
All inputs are finite; a program needn't handle non-finite values.
Results may differ from the reference program's by a relative error of at most 0.0034.
Values may be sent and summed in bfloat16 or wider, within the bound.
A program may use at most 64 MiB of HBM per device.

```python
import math
import jax
import jax.numpy as jnp
from jax import lax

BLOCK = 1024
KB = 2
STEPS = 10
TRIALS = 4
CAP = 128
AREAS = 4
RANKS = 8
NEURONS = 32768


def draw_tile_source(key, part):
    keys = jax.random.split(key, AREAS * KB)
    orders = jax.vmap(lambda single: jax.random.permutation(single, RANKS))(keys)
    return jnp.transpose(orders.reshape(AREAS, KB, RANKS), (0, 2, 1)).astype(jnp.int32)


def draw_send_count(key, part):
    first = jax.random.fold_in(key, 11)
    second = jax.random.fold_in(key, 12)
    third = jax.random.fold_in(key, 13)
    levels = jax.random.randint(first, (AREAS, 1, 1, 1), 1, 5)
    unclipped_spike_count = jax.random.randint(second, (AREAS, RANKS, AREAS, TRIALS), 0, CAP + 1)
    counts = jnp.minimum(unclipped_spike_count * levels // 2, CAP)
    spot = jax.random.randint(third, (), 0, AREAS * RANKS * AREAS * TRIALS)
    counts = counts.reshape(-1).at[spot].set(CAP)
    return counts.reshape(AREAS, RANKS, AREAS, TRIALS).astype(jnp.int32)


def with_ends(values, stream_key, least, top_value):
    index_at = [jax.random.randint(jax.random.fold_in(stream_key, axis), (), 0, length) for axis, length in enumerate(values.shape)]
    main_axis = values.shape.index(max(values.shape))
    neighbour = index_at[:main_axis] + [(index_at[main_axis] + 1) % values.shape[main_axis]] + index_at[main_axis + 1:]
    return values.at[tuple(index_at)].set(least).at[tuple(neighbour)].set(top_value)


def block_levels(stream_key, shape, pieces, least, high):
    loudness = 1.0
    for dim, parts in pieces:
        steps = jax.random.uniform(jax.random.fold_in(jax.random.fold_in(stream_key, 6), dim), (parts,), jnp.float32, least / len(pieces), high / len(pieces))
        loudness = loudness * jnp.repeat(jnp.exp(steps), shape[dim] // parts).reshape((-1,) + (1,) * (len(shape) - 1 - dim))
    return loudness


def scatter_about(own_key, extent, width, most, pieces=(), held_as=jnp.bfloat16):
    gain = block_levels(own_key, extent, pieces, -0.22, 0.18) if pieces else 1.0
    values = jax.random.normal(own_key, extent, jnp.float32) * width * gain
    return jnp.minimum(jnp.maximum(values, -most), most).astype(held_as)


def setup_inputs(seed: int = 0) -> dict:
    streams_of = jax.random.split(jax.random.key(seed), 14)
    membrane = scatter_about(streams_of[0], (TRIALS, NEURONS), 1.0, 6.0, ((1, 32),), jnp.float32)
    synaptic_trace = jnp.clip(2.0 * jax.random.uniform(streams_of[1], (TRIALS, NEURONS), jnp.float32) ** block_levels(streams_of[1], (TRIALS, NEURONS), ((1, 32),), -0.2, 0.2), 0.0, 2.0)
    pending = scatter_about(streams_of[2], (2, TRIALS, NEURONS), 1.0, 6.0, ((2, 32),), jnp.float32)
    inter_input = scatter_about(streams_of[3], (STEPS, TRIALS, NEURONS), 0.5, 4.0, ((2, 32),), jnp.float32)
    ext_spikes = with_ends(jax.random.randint(streams_of[4], (STEPS, TRIALS, NEURONS), 0, 4), jax.random.fold_in(streams_of[4], 1), 0, 3).astype(jnp.int32)
    mem_decay = jnp.clip(jnp.exp(math.log(0.95) - 0.4595323 * jax.random.uniform(streams_of[5], (NEURONS,), jnp.float32) ** block_levels(streams_of[5], (NEURONS,), ((0, 32),), -0.2, 0.2)), 0.6, 0.95)
    trace_decay_factor = jnp.clip(jnp.exp(math.log(0.8) - 0.98082923 * jax.random.uniform(streams_of[6], (NEURONS,), jnp.float32) ** block_levels(streams_of[6], (NEURONS,), ((0, 32),), -0.2, 0.2)), 0.3, 0.8)
    threshold = jnp.clip(0.5 + 1.0 * jax.random.uniform(streams_of[7], (NEURONS,), jnp.float32) ** block_levels(streams_of[7], (NEURONS,), ((0, 32),), -0.2, 0.2), 0.5, 1.5)
    weight_tiles = scatter_about(streams_of[8], (AREAS, RANKS, KB, BLOCK, BLOCK), (KB * BLOCK) ** -0.5, 0.125, ((0, 4), (1, 8)))
    tile_source = draw_tile_source(jax.random.fold_in(streams_of[13], 71), 0)
    send_amp = scatter_about(streams_of[10], (AREAS, RANKS, AREAS, TRIALS, CAP), 1.0, 6.0, ((0, 4), (1, 8)))
    send_target = with_ends(jax.random.randint(streams_of[11], (AREAS, RANKS, AREAS, TRIALS, CAP), 0, STEPS * BLOCK), jax.random.fold_in(streams_of[11], 1), 0, (STEPS * BLOCK) - 1).astype(jnp.int32)
    send_count = draw_send_count(jax.random.fold_in(streams_of[13], 71), 0)
    return dict(membrane=membrane, synaptic_trace=synaptic_trace, pending=pending, inter_input=inter_input, ext_spikes=ext_spikes, mem_decay=mem_decay, trace_decay_factor=trace_decay_factor, threshold=threshold, weight_tiles=weight_tiles, tile_source=tile_source, send_amp=send_amp, send_target=send_target, send_count=send_count)


def intra_current(sent_trace, weight_tiles, tile_source):
    blocks = sent_trace.reshape(TRIALS, AREAS * RANKS, BLOCK)
    flat_tiles = weight_tiles.reshape(AREAS * RANKS, KB, BLOCK, BLOCK)
    sources = tile_source.reshape(AREAS * RANKS, KB)
    owners = jnp.arange(AREAS * RANKS, dtype=jnp.int32)

    def one_device(inputs):
        dev_tiles, dev_src, owner = inputs
        area_start = (owner // RANKS) * RANKS
        summed = jnp.zeros((TRIALS, BLOCK), jnp.float32)
        for tile_slot in range(KB):
            source_block = lax.dynamic_index_in_dim(blocks, (area_start + dev_src[tile_slot]).astype(jnp.int32), axis=1, keepdims=False)
            summed = summed + jnp.dot(source_block, dev_tiles[tile_slot], preferred_element_type=jnp.float32)
        return summed

    per_device = lax.map(one_device, (flat_tiles, sources, owners))
    return jnp.transpose(per_device, (1, 0, 2)).reshape(TRIALS, AREAS * RANKS * BLOCK)


def deliver(send_amp, send_target, send_count):
    in_list = jnp.arange(CAP, dtype=jnp.int32) < send_count[..., None]
    values = jnp.where(in_list, send_amp.astype(jnp.float32), jnp.float32(0.0))
    delay_step = send_target // BLOCK
    local_cell = send_target % BLOCK
    dest_area = jnp.arange(AREAS, dtype=jnp.int32)[None, None, :, None, None]
    rank_index = jnp.arange(RANKS, dtype=jnp.int32)[None, :, None, None, None]
    trial_index = jnp.arange(TRIALS, dtype=jnp.int32)[None, None, None, :, None]
    neuron = (dest_area * RANKS + rank_index) * BLOCK + local_cell
    flat_index = (delay_step * TRIALS + trial_index) * (AREAS * RANKS * BLOCK) + neuron
    result = jnp.zeros((STEPS * TRIALS * AREAS * RANKS * BLOCK,), jnp.float32)
    result = result.at[flat_index.reshape(-1)].add(values.reshape(-1))
    return result.reshape(STEPS, TRIALS, AREAS * RANKS * BLOCK)


def reference(membrane, synaptic_trace, pending, inter_input, ext_spikes, mem_decay, trace_decay_factor, threshold, weight_tiles, tile_source, send_amp, send_target, send_count):
    membrane_voltage = membrane
    synaptic_trace_state = synaptic_trace
    currents = [pending[0], pending[1]] + [None] * (STEPS - 2)
    history = []
    for step_index in range(STEPS):
        drive_now = (currents[step_index] + inter_input[step_index]) + 0.25 * ext_spikes[step_index].astype(jnp.float32)
        membrane_voltage = mem_decay * membrane_voltage + drive_now
        spike_flags = jax.nn.sigmoid(4.0 * (membrane_voltage - threshold))
        membrane_voltage = membrane_voltage * (1.0 - spike_flags)
        synaptic_trace_state = trace_decay_factor * synaptic_trace_state + spike_flags
        sent_trace = synaptic_trace_state.astype(jnp.bfloat16)
        history.append(sent_trace)
        if step_index + 2 < STEPS:
            currents[step_index + 2] = intra_current(sent_trace, weight_tiles, tile_source)
    late_traces = jnp.stack([history[STEPS - 2], history[STEPS - 1]])
    delivered = deliver(send_amp, send_target, send_count)
    return membrane_voltage, synaptic_trace_state, late_traces, delivered
```

```python
import functools

import jax
import jax.numpy as jnp
from jax import lax
from jax.experimental import pallas as pl
from jax.experimental.pallas import tpu as pltpu
from jax.sharding import PartitionSpec as P

MESH = pl.DeviceIdType.MESH


def peer_orders(count):
    core = 2 if count % 2 == 0 else 1
    inner = 2 if count % (2 * core) == 0 else 1
    outer = count // (core * inner)
    offsets = [(a, b, c) for a in range(outer) for b in range(inner) for c in range(core)]
    offsets = [o for o in offsets if o != (0, 0, 0)]
    offsets.sort(key=lambda o: -((o[0] != 0) + (o[1] != 0)))
    return (outer, inner, core), offsets


def peer_of(me, sizes, offset):
    outer, inner, core = sizes
    a = (me // (inner * core) + offset[0]) % outer
    b = (me // core % inner + offset[1]) % inner
    c = (me % core + offset[2]) % core
    return (a * inner + b) * core + c


def kernel(areas, ranks, steps, *refs):
    (membrane, trace, pending, inter, ext, decay, trace_decay, threshold, weights, tile_source,
     amp, target, count) = refs[:13]
    voltage_out, trace_out, late_out, delivered_out = refs[13:17]
    (v_in, s_in, pend, inter_v, ext_v, decay_v, td_v, th_v, w_v, src_s, got_amp, got_target, got_count,
     load_sem, send_sem, recv_sem, list_send, list_recv) = refs[17:35]
    frames = refs[35:]
    sends = steps - 2
    trials, block = membrane.shape
    tiles = weights.shape[2]
    rank = lax.axis_index("rank")
    area = lax.axis_index("area")
    sizes, offsets = peer_orders(ranks)

    barrier = pltpu.get_barrier_semaphore()
    for offset in offsets:
        pl.semaphore_signal(barrier, 1, device_id={"rank": peer_of(rank, sizes, offset)}, device_id_type=MESH)
    for shift in range(1, areas):
        pl.semaphore_signal(barrier, 1, device_id={"area": lax.rem(area + shift, areas)}, device_id_type=MESH)

    loads = [
        (membrane, v_in), (trace, s_in), (pending, pend), (inter, inter_v), (ext, ext_v),
        (decay, decay_v), (trace_decay, td_v), (threshold, th_v), (tile_source, src_s),
        (amp.at[0, 0, area], got_amp.at[area]), (target.at[0, 0, area], got_target.at[area]),
        (count.at[0, 0], got_count.at[area]),
    ] + [(weights.at[0, 0, k], w_v.at[pl.ds(k * block, block)]) for k in range(tiles)]
    copies = [pltpu.make_async_copy(a, b, load_sem.at[n]) for n, (a, b) in enumerate(loads)]
    for copy in copies:
        copy.start()
    for copy in copies[:8]:
        copy.wait()

    shape = (trials, block)
    m_decay = jnp.broadcast_to(decay_v[...], shape)
    t_decay = jnp.broadcast_to(td_v[...], shape)
    limit = jnp.broadcast_to(th_v[...], shape)

    def advance(t, v, s, current):
        drive = current + (inter_v[t] + 0.25 * ext_v[t].astype(jnp.float32))
        v = m_decay * v + drive
        firing = 1.0 / (1.0 + jnp.exp(-4.0 * (v - limit)))
        return v * (1.0 - firing), t_decay * s + firing

    def send(t, s):
        frames[t][rank] = s.astype(jnp.bfloat16)
        if t == 0:
            pl.semaphore_wait(barrier, ranks + areas - 2)
        started = []
        for offset in offsets:
            started.append(pltpu.make_async_remote_copy(
                src_ref=frames[t].at[rank], dst_ref=frames[t].at[rank],
                send_sem=send_sem.at[t], recv_sem=recv_sem.at[t],
                device_id={"rank": peer_of(rank, sizes, offset)}, device_id_type=MESH))
        for copy in started:
            copy.start()

    def all_of(t, sem):
        part = frames[t].at[pl.ds(0, ranks - 1)]
        return pltpu.make_async_copy(part, part, sem.at[t])

    v, s = advance(0, v_in[...], s_in[...], pend[0])
    send(0, s)
    lists = []
    for shift in range(1, areas):
        other = lax.rem(area + shift, areas)
        for n, (a, b) in enumerate((
            (amp.at[0, 0, other], got_amp.at[area]), (target.at[0, 0, other], got_target.at[area]),
            (count.at[0, 0], got_count.at[area]),
        )):
            lists.append(pltpu.make_async_remote_copy(
                src_ref=a, dst_ref=b, send_sem=list_send.at[shift, n], recv_sem=list_recv.at[shift, n],
                device_id={"area": other}, device_id_type=MESH))
    v, s = advance(1, v, s, pend[1])
    send(1, s)
    for copy in lists:
        copy.start()
    for copy in copies[8:]:
        copy.wait()
    source = [src_s[0, 0, k] for k in range(tiles)]

    def deliver():
        for copy in lists:
            copy.wait()
        width = got_amp.shape[2]
        lanes = 128
        groups = block // lanes
        rows = groups * steps * trials
        eye = lax.broadcasted_iota(jnp.int32, (trials, trials), 0) == lax.broadcasted_iota(
            jnp.int32, (trials, trials), 1)
        mine = lax.broadcasted_iota(jnp.int32, (areas, trials), 0) == area
        slot = lax.broadcasted_iota(jnp.int32, (trials, width), 1)
        trial = lax.broadcasted_iota(jnp.int32, (trials, width), 0)
        row_id = lax.broadcasted_iota(jnp.int32, (rows, width), 0)
        lane_id = lax.broadcasted_iota(jnp.int32, (lanes, width), 0)
        total = None
        for a in range(areas):
            live = jnp.sum(jnp.where(mine, got_count[a].astype(jnp.float32), 0.0), axis=0, keepdims=True)
            live = jnp.sum(jnp.where(eye, jnp.broadcast_to(live, (trials, trials)), 0.0), axis=1, keepdims=True)
            value = jnp.where(slot < live.astype(jnp.int32), got_amp[a].astype(jnp.float32), 0.0)
            g = got_target[a]
            cell = g % block
            key = (cell // lanes) * (steps * trials) + (g // block) * trials + trial
            low = cell % lanes
            left, right = [], []
            for i in range(trials):
                left.append(jnp.where(row_id == key[i:i + 1], value[i:i + 1], 0.0).astype(jnp.bfloat16))
                right.append(jnp.where(lane_id == low[i:i + 1], 1.0, 0.0).astype(jnp.bfloat16))
            part = lax.dot_general(
                jnp.concatenate(left, axis=1), jnp.concatenate(right, axis=1), (((1,), (1,)), ((), ())),
                preferred_element_type=jnp.float32)
            total = part if total is None else total + part
        for c in range(groups):
            for d in range(steps):
                r = (c * steps + d) * trials
                delivered_out[d, :, c * lanes:(c + 1) * lanes] = total[r:r + trials]

    for t in range(2, steps):
        all_of(t - 2, recv_sem).wait()
        chosen = jnp.concatenate([frames[t - 2][src] for src in source], axis=1)
        current = jnp.dot(chosen, w_v[...], preferred_element_type=jnp.float32)
        v, s = advance(t, v, s, current)
        if t < sends:
            send(t, s)
        else:
            late_out[t - sends] = s.astype(jnp.bfloat16)
        if t == 3:
            deliver()
    voltage_out[...] = v
    trace_out[...] = s
    for t in range(sends):
        all_of(t, send_sem).wait()


def on_device(areas, ranks, *args):
    (membrane, synaptic_trace, pending, inter_input, ext_spikes, mem_decay, trace_decay_factor, threshold,
     weight_tiles, tile_source, send_amp, send_target, send_count) = args
    trials, block = membrane.shape
    steps = inter_input.shape[0]
    tiles = weight_tiles.shape[2]
    width = send_amp.shape[4]
    f32, i32, bf16 = jnp.float32, jnp.int32, jnp.bfloat16
    vmem = pltpu.VMEM
    dma = pltpu.SemaphoreType.DMA
    return pl.pallas_call(
        functools.partial(kernel, areas, ranks, steps),
        out_shape=(
            jax.ShapeDtypeStruct((trials, block), f32),
            jax.ShapeDtypeStruct((trials, block), f32),
            jax.ShapeDtypeStruct((2, trials, block), bf16),
            jax.ShapeDtypeStruct((steps, trials, block), f32),
        ),
        in_specs=[pl.BlockSpec(memory_space=pl.ANY)] * 13,
        out_specs=(pl.BlockSpec(memory_space=pltpu.VMEM),) * 4,
        scratch_shapes=[
            vmem((trials, block), f32), vmem((trials, block), f32), vmem((2, trials, block), f32),
            vmem((steps, trials, block), f32), vmem((steps, trials, block), i32),
            vmem((1, block), f32), vmem((1, block), f32), vmem((1, block), f32),
            vmem((tiles * block, block), bf16), pltpu.SMEM((1, 1, tiles), i32),
            vmem((areas, trials, width), bf16), vmem((areas, trials, width), i32),
            vmem((areas, areas, trials), i32),
            dma((12 + tiles,)), dma((steps - 2,)), dma((steps - 2,)),
            dma((areas, 3)), dma((areas, 3)),
        ] + [vmem((ranks, trials, block), bf16) for _ in range(steps - 2)],
        compiler_params=pltpu.CompilerParams(collective_id=0, has_side_effects=True),
    )(membrane, synaptic_trace, pending, inter_input, ext_spikes, mem_decay.reshape(1, block),
      trace_decay_factor.reshape(1, block), threshold.reshape(1, block), weight_tiles, tile_source,
      send_amp, send_target, send_count)


def solution(mesh):
    both = ("area", "rank")
    placed = (
        P(None, both), P(None, both), P(None, None, both), P(None, None, both), P(None, None, both),
        P(both), P(both), P(both), P("area", "rank", None, None, None), P("area", "rank", None),
        P("area", "rank", None, None, None), P("area", "rank", None, None, None),
        P("area", "rank", None, None),
    )
    return jax.shard_map(
        functools.partial(on_device, mesh.shape["area"], mesh.shape["rank"]),
        mesh=mesh,
        in_specs=placed,
        out_specs=(P(None, both), P(None, both), P(None, None, both), P(None, None, both)),
        check_vma=False,
    )
```

```python
import functools

import jax
import jax.numpy as jnp
from jax import lax
from jax.experimental import pallas as pl
from jax.experimental.pallas import tpu as pltpu
from jax.sharding import PartitionSpec as P

MESH = pl.DeviceIdType.MESH


def peer_orders(count):
    core = 2 if count % 2 == 0 else 1
    inner = 2 if count % (2 * core) == 0 else 1
    outer = count // (core * inner)
    offsets = [(a, b, c) for a in range(outer) for b in range(inner) for c in range(core)]
    offsets = [o for o in offsets if o != (0, 0, 0)]
    offsets.sort(key=lambda o: -((o[0] != 0) + (o[1] != 0)))
    return (outer, inner, core), offsets


def peer_of(me, sizes, offset):
    outer, inner, core = sizes
    a = (me // (inner * core) + offset[0]) % outer
    b = (me // core % inner + offset[1]) % inner
    c = (me % core + offset[2]) % core
    return (a * inner + b) * core + c


def kernel(areas, ranks, steps, *refs):
    (membrane, trace, pending, inter, ext, decay, trace_decay, threshold, weights, tile_source,
     amp, target, count) = refs[:13]
    voltage_out, trace_out, late_out, delivered_out = refs[13:17]
    (v_in, s_in, pend, inter_v, ext_v, decay_v, td_v, th_v, w_v, src_s, got_amp, got_target, got_count,
     load_sem, send_sem, recv_sem, list_send, list_recv) = refs[17:35]
    frames = refs[35:]
    sends = steps - 2
    trials, block = membrane.shape
    tiles = weights.shape[2]
    rank = lax.axis_index("rank")
    area = lax.axis_index("area")
    sizes, offsets = peer_orders(ranks)

    barrier = pltpu.get_barrier_semaphore()
    for offset in offsets:
        pl.semaphore_signal(barrier, 1, device_id={"rank": peer_of(rank, sizes, offset)}, device_id_type=MESH)
    for shift in range(1, areas):
        pl.semaphore_signal(barrier, 1, device_id={"area": lax.rem(area + shift, areas)}, device_id_type=MESH)

    loads = [
        (membrane, v_in), (trace, s_in), (pending, pend), (inter, inter_v), (ext, ext_v),
        (decay, decay_v), (trace_decay, td_v), (threshold, th_v), (tile_source, src_s),
        (amp.at[0, 0, area], got_amp.at[area]), (target.at[0, 0, area], got_target.at[area]),
        (count.at[0, 0], got_count.at[area]),
    ] + [(weights.at[0, 0, k], w_v.at[pl.ds(k * block, block)]) for k in range(tiles)]
    copies = [pltpu.make_async_copy(a, b, load_sem.at[n]) for n, (a, b) in enumerate(loads)]
    for copy in copies:
        copy.start()
    for copy in copies[:8]:
        copy.wait()

    shape = (trials, block)
    m_decay = jnp.broadcast_to(decay_v[...], shape)
    t_decay = jnp.broadcast_to(td_v[...], shape)
    limit = jnp.broadcast_to(th_v[...], shape)

    def advance(t, v, s, current):
        drive = current + (inter_v[t] + 0.25 * ext_v[t].astype(jnp.float32))
        v = m_decay * v + drive
        firing = 1.0 / (1.0 + jnp.exp(-4.0 * (v - limit)))
        return v * (1.0 - firing), t_decay * s + firing

    def send(t, s):
        frames[t][rank] = s.astype(jnp.bfloat16)
        if t == 0:
            pl.semaphore_wait(barrier, ranks + areas - 2)
        started = []
        for offset in offsets:
            started.append(pltpu.make_async_remote_copy(
                src_ref=frames[t].at[rank], dst_ref=frames[t].at[rank],
                send_sem=send_sem.at[t], recv_sem=recv_sem.at[t],
                device_id={"rank": peer_of(rank, sizes, offset)}, device_id_type=MESH))
        for copy in started:
            copy.start()

    def all_of(t, sem):
        part = frames[t].at[pl.ds(0, ranks - 1)]
        return pltpu.make_async_copy(part, part, sem.at[t])

    v, s = advance(0, v_in[...], s_in[...], pend[0])
    send(0, s)
    lists = []
    for shift in range(1, areas):
        other = lax.rem(area + shift, areas)
        for n, (a, b) in enumerate((
            (amp.at[0, 0, other], got_amp.at[area]), (target.at[0, 0, other], got_target.at[area]),
            (count.at[0, 0], got_count.at[area]),
        )):
            lists.append(pltpu.make_async_remote_copy(
                src_ref=a, dst_ref=b, send_sem=list_send.at[shift, n], recv_sem=list_recv.at[shift, n],
                device_id={"area": other}, device_id_type=MESH))
    v, s = advance(1, v, s, pend[1])
    send(1, s)
    for copy in lists:
        copy.start()
    for copy in copies[8:]:
        copy.wait()
    source = [src_s[0, 0, k] for k in range(tiles)]

    def deliver():
        for copy in lists:
            copy.wait()
        width = got_amp.shape[2]
        lanes = 128
        groups = block // lanes
        rows = groups * steps * trials
        eye = lax.broadcasted_iota(jnp.int32, (trials, trials), 0) == lax.broadcasted_iota(
            jnp.int32, (trials, trials), 1)
        mine = lax.broadcasted_iota(jnp.int32, (areas, trials), 0) == area
        slot = lax.broadcasted_iota(jnp.int32, (trials, width), 1)
        trial = lax.broadcasted_iota(jnp.int32, (trials, width), 0)
        row_id = lax.broadcasted_iota(jnp.int32, (rows, width), 0)
        lane_id = lax.broadcasted_iota(jnp.int32, (lanes, width), 0)
        total = None
        for a in range(areas):
            live = jnp.sum(jnp.where(mine, got_count[a].astype(jnp.float32), 0.0), axis=0, keepdims=True)
            live = jnp.sum(jnp.where(eye, jnp.broadcast_to(live, (trials, trials)), 0.0), axis=1, keepdims=True)
            value = jnp.where(slot < live.astype(jnp.int32), got_amp[a].astype(jnp.float32), 0.0)
            g = got_target[a]
            cell = g % block
            key = (cell // lanes) * (steps * trials) + (g // block) * trials + trial
            low = cell % lanes
            left, right = [], []
            for i in range(trials):
                left.append(jnp.where(row_id == key[i:i + 1], value[i:i + 1], 0.0).astype(jnp.bfloat16))
                right.append(jnp.where(lane_id == low[i:i + 1], 1.0, 0.0).astype(jnp.bfloat16))
            part = lax.dot_general(
                jnp.concatenate(left, axis=1), jnp.concatenate(right, axis=1), (((1,), (1,)), ((), ())),
                preferred_element_type=jnp.float32)
            total = part if total is None else total + part
        for c in range(groups):
            for d in range(steps):
                r = (c * steps + d) * trials
                delivered_out[d, :, c * lanes:(c + 1) * lanes] = total[r:r + trials]

    for t in range(2, steps):
        all_of(t - 2, recv_sem).wait()
        chosen = jnp.concatenate([frames[t - 2][src] for src in source], axis=1)
        current = jnp.dot(chosen, w_v[...], preferred_element_type=jnp.float32)
        v, s = advance(t, v, s, current)
        if t < sends:
            send(t, s)
        else:
            late_out[t - sends] = s.astype(jnp.bfloat16)
        if t == 3:
            deliver()
    voltage_out[...] = v
    trace_out[...] = s
    for t in range(sends):
        all_of(t, send_sem).wait()


def hand_over(*refs):
    sems = refs[8]
    copies = [pltpu.make_async_copy(refs[n], refs[4 + n], sems.at[n]) for n in range(4)]
    for copy in copies:
        copy.start()
    for copy in copies:
        copy.wait()


def on_device(areas, ranks, *args):
    (membrane, synaptic_trace, pending, inter_input, ext_spikes, mem_decay, trace_decay_factor, threshold,
     weight_tiles, tile_source, send_amp, send_target, send_count) = args
    trials, block = membrane.shape
    steps = inter_input.shape[0]
    tiles = weight_tiles.shape[2]
    width = send_amp.shape[4]
    f32, i32, bf16 = jnp.float32, jnp.int32, jnp.bfloat16
    vmem = pltpu.VMEM
    dma = pltpu.SemaphoreType.DMA
    shapes = (
        jax.ShapeDtypeStruct((trials, block), f32),
        jax.ShapeDtypeStruct((trials, block), f32),
        jax.ShapeDtypeStruct((2, trials, block), bf16),
        jax.ShapeDtypeStruct((steps, trials, block), f32),
    )
    results = pl.pallas_call(
        functools.partial(kernel, areas, ranks, steps),
        out_shape=tuple(vmem(x.shape, x.dtype) for x in shapes),
        in_specs=[pl.BlockSpec(memory_space=pltpu.HBM)] * 13,
        out_specs=(pl.BlockSpec(memory_space=pltpu.VMEM),) * 4,
        scratch_shapes=[
            vmem((trials, block), f32), vmem((trials, block), f32), vmem((2, trials, block), f32),
            vmem((steps, trials, block), f32), vmem((steps, trials, block), i32),
            vmem((1, block), f32), vmem((1, block), f32), vmem((1, block), f32),
            vmem((tiles * block, block), bf16), pltpu.SMEM((1, 1, tiles), i32),
            vmem((areas, trials, width), bf16), vmem((areas, trials, width), i32),
            vmem((areas, areas, trials), i32),
            dma((12 + tiles,)), dma((steps - 2,)), dma((steps - 2,)),
            dma((areas, 3)), dma((areas, 3)),
        ] + [vmem((ranks, trials, block), bf16) for _ in range(steps - 2)],
        compiler_params=pltpu.CompilerParams(collective_id=0, has_side_effects=True),
    )(membrane, synaptic_trace, pending, inter_input, ext_spikes, mem_decay.reshape(1, block),
      trace_decay_factor.reshape(1, block), threshold.reshape(1, block), weight_tiles, tile_source,
      send_amp, send_target, send_count)
    return pl.pallas_call(
        hand_over,
        out_shape=shapes,
        in_specs=[pl.BlockSpec(memory_space=pl.ANY)] * 4,
        out_specs=(pl.BlockSpec(memory_space=pltpu.HBM),) * 4,
        scratch_shapes=[dma((4,))],
        compiler_params=pltpu.CompilerParams(vmem_limit_bytes=1 << 20),
    )(*results)


def solution(mesh):
    both = ("area", "rank")
    placed = (
        P(None, both), P(None, both), P(None, None, both), P(None, None, both), P(None, None, both),
        P(both), P(both), P(both), P("area", "rank", None, None, None), P("area", "rank", None),
        P("area", "rank", None, None, None), P("area", "rank", None, None, None),
        P("area", "rank", None, None),
    )
    return jax.shard_map(
        functools.partial(on_device, mesh.shape["area"], mesh.shape["rank"]),
        mesh=mesh,
        in_specs=placed,
        out_specs=(P(None, both), P(None, both), P(None, None, both), P(None, None, both)),
        check_vma=False,
    )
```

```python
import functools

import jax
import jax.numpy as jnp
from jax import lax
from jax.experimental import pallas as pl
from jax.experimental.pallas import tpu as pltpu
from jax.sharding import PartitionSpec as P

MESH = pl.DeviceIdType.MESH


def peer_orders(count):
    core = 2 if count % 2 == 0 else 1
    inner = 2 if count % (2 * core) == 0 else 1
    outer = count // (core * inner)
    offsets = [(a, b, c) for a in range(outer) for b in range(inner) for c in range(core)]
    offsets = [o for o in offsets if o != (0, 0, 0)]
    offsets.sort(key=lambda o: -((o[0] != 0) + (o[1] != 0)))
    return (outer, inner, core), offsets


def peer_of(me, sizes, offset):
    outer, inner, core = sizes
    a = (me // (inner * core) + offset[0]) % outer
    b = (me // core % inner + offset[1]) % inner
    c = (me % core + offset[2]) % core
    return (a * inner + b) * core + c


def kernel(areas, ranks, steps, *refs):
    (membrane, trace, pending, inter, ext, decay, trace_decay, threshold, weights, tile_source,
     amp, target, count) = refs[:13]
    voltage_out, trace_out, late_out, delivered_out = refs[13:17]
    (v_in, s_in, pend, inter_v, ext_v, decay_v, td_v, th_v, w_v, src_s, got_amp, got_target, got_count,
     load_sem, send_sem, recv_sem, list_send, list_recv) = refs[17:35]
    frames = refs[35:]
    sends = steps - 2
    trials, block = membrane.shape
    tiles = weights.shape[2]
    rank = lax.axis_index("rank")
    area = lax.axis_index("area")
    sizes, offsets = peer_orders(ranks)

    barrier = pltpu.get_barrier_semaphore()
    for offset in offsets:
        pl.semaphore_signal(barrier, 1, device_id={"rank": peer_of(rank, sizes, offset)}, device_id_type=MESH)
    for near in (-1, 1):
        @pl.when((area + near >= 0) & (area + near < areas))
        def _():
            pl.semaphore_signal(barrier, 1, device_id={"area": (area + near + areas) % areas}, device_id_type=MESH)
    neighbours = (area + areas - 1) // areas + (2 * areas - 2 - area) // areas

    loads = [
        (membrane, v_in), (trace, s_in), (pending, pend), (inter, inter_v), (ext, ext_v),
        (decay, decay_v), (trace_decay, td_v), (threshold, th_v), (tile_source, src_s),
        (amp.at[0, 0], got_amp.at[area]), (target.at[0, 0], got_target.at[area]),
        (count.at[0, 0], got_count.at[area]),
    ] + [(weights.at[0, 0, k], w_v.at[pl.ds(k * block, block)]) for k in range(tiles)]
    copies = [pltpu.make_async_copy(a, b, load_sem.at[n]) for n, (a, b) in enumerate(loads)]
    for copy in copies:
        copy.start()
    for copy in copies[:8]:
        copy.wait()

    shape = (trials, block)
    m_decay = jnp.broadcast_to(decay_v[...], shape)
    t_decay = jnp.broadcast_to(td_v[...], shape)
    limit = jnp.broadcast_to(th_v[...], shape)

    def advance(t, v, s, current):
        drive = current + (inter_v[t] + 0.25 * ext_v[t].astype(jnp.float32))
        v = m_decay * v + drive
        firing = 1.0 / (1.0 + jnp.exp(-4.0 * (v - limit)))
        return v * (1.0 - firing), t_decay * s + firing

    def send(t, s):
        frames[t][rank] = s.astype(jnp.bfloat16)
        if t == 0:
            pl.semaphore_wait(barrier, ranks - 1 + neighbours)
        started = []
        for offset in offsets:
            started.append(pltpu.make_async_remote_copy(
                src_ref=frames[t].at[rank], dst_ref=frames[t].at[rank],
                send_sem=send_sem.at[t], recv_sem=recv_sem.at[t],
                device_id={"rank": peer_of(rank, sizes, offset)}, device_id_type=MESH))
        for copy in started:
            copy.start()

    def all_of(t, sem):
        part = frames[t].at[pl.ds(0, ranks - 1)]
        return pltpu.make_async_copy(part, part, sem.at[t])

    v, s = advance(0, v_in[...], s_in[...], pend[0])
    send(0, s)
    v, s = advance(1, v, s, pend[1])
    send(1, s)
    for copy in copies[8:]:
        copy.wait()
    source = [src_s[0, 0, k] for k in range(tiles)]

    def passing(owner, near):
        other = (area + near + areas) % areas
        return [pltpu.make_async_remote_copy(
            src_ref=box.at[owner], dst_ref=box.at[owner], send_sem=list_send.at[owner, (1 - near) // 2, n],
            recv_sem=list_recv.at[owner, n], device_id={"area": other}, device_id_type=MESH)
            for n, box in enumerate((got_amp, got_target, got_count))]

    def hop(distance, act):
        for near in (-1, 1):
            owner = area - near * (distance - 1)
            inside = (owner >= 0) & (owner < areas) & (area + near >= 0) & (area + near < areas)

            @pl.when(inside)
            def _():
                for copy in passing((owner + areas) % areas, near):
                    act(copy)

    def arrived(distance):
        for near in (-1, 1):
            owner = area - near * distance

            @pl.when((owner >= 0) & (owner < areas))
            def _():
                for copy in passing((owner + areas) % areas, near):
                    copy.wait_recv()

    def exchange(distance):
        if distance > 1:
            arrived(distance - 1)
        hop(distance, lambda copy: copy.start())

    def deliver():
        width = got_amp.shape[3]
        lanes = 128
        groups = block // lanes
        rows = groups * steps * trials
        eye = lax.broadcasted_iota(jnp.int32, (trials, trials), 0) == lax.broadcasted_iota(
            jnp.int32, (trials, trials), 1)
        mine = lax.broadcasted_iota(jnp.int32, (areas, trials), 0) == area
        slot = lax.broadcasted_iota(jnp.int32, (trials, width), 1)
        trial = lax.broadcasted_iota(jnp.int32, (trials, width), 0)
        row_id = lax.broadcasted_iota(jnp.int32, (rows, width), 0)
        lane_id = lax.broadcasted_iota(jnp.int32, (lanes, width), 0)
        total = None
        for a in range(areas):
            live = jnp.sum(jnp.where(mine, got_count[a].astype(jnp.float32), 0.0), axis=0, keepdims=True)
            live = jnp.sum(jnp.where(eye, jnp.broadcast_to(live, (trials, trials)), 0.0), axis=1, keepdims=True)
            value = jnp.where(slot < live.astype(jnp.int32), got_amp[a, area].astype(jnp.float32), 0.0)
            g = got_target[a, area]
            cell = g % block
            key = (cell // lanes) * (steps * trials) + (g // block) * trials + trial
            low = cell % lanes
            left, right = [], []
            for i in range(trials):
                left.append(jnp.where(row_id == key[i:i + 1], value[i:i + 1], 0.0).astype(jnp.bfloat16))
                right.append(jnp.where(lane_id == low[i:i + 1], 1.0, 0.0).astype(jnp.bfloat16))
            part = lax.dot_general(
                jnp.concatenate(left, axis=1), jnp.concatenate(right, axis=1), (((1,), (1,)), ((), ())),
                preferred_element_type=jnp.float32)
            total = part if total is None else total + part
        for c in range(groups):
            for d in range(steps):
                r = (c * steps + d) * trials
                delivered_out[d, :, c * lanes:(c + 1) * lanes] = total[r:r + trials]

    exchange(1)
    for t in range(2, steps):
        all_of(t - 2, recv_sem).wait()
        chosen = jnp.concatenate([frames[t - 2][src] for src in source], axis=1)
        current = jnp.dot(chosen, w_v[...], preferred_element_type=jnp.float32)
        v, s = advance(t, v, s, current)
        if t < sends:
            send(t, s)
        else:
            late_out[t - sends] = s.astype(jnp.bfloat16)
        if t < steps - 3 and t < areas:
            exchange(t)
        if t == steps - 4:
            for distance in range(steps - 3, areas):
                exchange(distance)
            arrived(areas - 1)
            deliver()
    voltage_out[...] = v
    trace_out[...] = s
    for t in range(sends):
        all_of(t, send_sem).wait()
    for distance in range(1, areas):
        hop(distance, lambda copy: copy.wait_send())


def hand_over(*refs):
    sems = refs[8]
    copies = [pltpu.make_async_copy(refs[n], refs[4 + n], sems.at[n]) for n in range(4)]
    for copy in copies:
        copy.start()
    for copy in copies:
        copy.wait()


def on_device(areas, ranks, *args):
    (membrane, synaptic_trace, pending, inter_input, ext_spikes, mem_decay, trace_decay_factor, threshold,
     weight_tiles, tile_source, send_amp, send_target, send_count) = args
    trials, block = membrane.shape
    steps = inter_input.shape[0]
    tiles = weight_tiles.shape[2]
    width = send_amp.shape[4]
    f32, i32, bf16 = jnp.float32, jnp.int32, jnp.bfloat16
    vmem = pltpu.VMEM
    dma = pltpu.SemaphoreType.DMA
    shapes = (
        jax.ShapeDtypeStruct((trials, block), f32),
        jax.ShapeDtypeStruct((trials, block), f32),
        jax.ShapeDtypeStruct((2, trials, block), bf16),
        jax.ShapeDtypeStruct((steps, trials, block), f32),
    )
    results = pl.pallas_call(
        functools.partial(kernel, areas, ranks, steps),
        out_shape=tuple(vmem(x.shape, x.dtype) for x in shapes),
        in_specs=[pl.BlockSpec(memory_space=pltpu.HBM)] * 13,
        out_specs=(pl.BlockSpec(memory_space=pltpu.VMEM),) * 4,
        scratch_shapes=[
            vmem((trials, block), f32), vmem((trials, block), f32), vmem((2, trials, block), f32),
            vmem((steps, trials, block), f32), vmem((steps, trials, block), i32),
            vmem((1, block), f32), vmem((1, block), f32), vmem((1, block), f32),
            vmem((tiles * block, block), bf16), pltpu.SMEM((1, 1, tiles), i32),
            vmem((areas, areas, trials, width), bf16), vmem((areas, areas, trials, width), i32),
            vmem((areas, areas, trials), i32),
            dma((12 + tiles,)), dma((steps - 2,)), dma((steps - 2,)),
            dma((areas, 2, 3)), dma((areas, 3)),
        ] + [vmem((ranks, trials, block), bf16) for _ in range(steps - 2)],
        compiler_params=pltpu.CompilerParams(collective_id=0, has_side_effects=True),
    )(membrane, synaptic_trace, pending, inter_input, ext_spikes, mem_decay.reshape(1, block),
      trace_decay_factor.reshape(1, block), threshold.reshape(1, block), weight_tiles, tile_source,
      send_amp, send_target, send_count)
    return pl.pallas_call(
        hand_over,
        out_shape=shapes,
        in_specs=[pl.BlockSpec(memory_space=pl.ANY)] * 4,
        out_specs=(pl.BlockSpec(memory_space=pltpu.HBM),) * 4,
        scratch_shapes=[dma((4,))],
        compiler_params=pltpu.CompilerParams(vmem_limit_bytes=1 << 20),
    )(*results)


def solution(mesh):
    both = ("area", "rank")
    placed = (
        P(None, both), P(None, both), P(None, None, both), P(None, None, both), P(None, None, both),
        P(both), P(both), P(both), P("area", "rank", None, None, None), P("area", "rank", None),
        P("area", "rank", None, None, None), P("area", "rank", None, None, None),
        P("area", "rank", None, None),
    )
    return jax.shard_map(
        functools.partial(on_device, mesh.shape["area"], mesh.shape["rank"]),
        mesh=mesh,
        in_specs=placed,
        out_specs=(P(None, both), P(None, both), P(None, None, both), P(None, None, both)),
        check_vma=False,
    )
```

```python
import functools

import jax
import jax.numpy as jnp
from jax import lax
from jax.experimental import pallas as pl
from jax.experimental.pallas import tpu as pltpu
from jax.sharding import PartitionSpec as P

MESH = pl.DeviceIdType.MESH


def peer_orders(count):
    core = 2 if count % 2 == 0 else 1
    inner = 2 if count % (2 * core) == 0 else 1
    outer = count // (core * inner)
    offsets = [(a, b, c) for a in range(outer) for b in range(inner) for c in range(core)]
    offsets = [o for o in offsets if o != (0, 0, 0)]
    offsets.sort(key=lambda o: -((o[0] != 0) + (o[1] != 0)))
    return (outer, inner, core), offsets


def peer_of(me, sizes, offset):
    outer, inner, core = sizes
    a = (me // (inner * core) + offset[0]) % outer
    b = (me // core % inner + offset[1]) % inner
    c = (me % core + offset[2]) % core if offset[:2] == (0, 0) else offset[2]
    return (a * inner + b) * core + c


def kernel(areas, ranks, steps, *refs):
    (membrane, trace, pending, inter, ext, decay, trace_decay, threshold, weights, tile_source,
     amp, target, count) = refs[:13]
    voltage_out, trace_out, late_out, delivered_out = refs[13:17]
    (v_in, s_in, pend, inter_v, ext_v, decay_v, td_v, th_v, w_v, src_s, got_amp, got_target, got_count,
     load_sem, send_sem, recv_sem, list_send, list_recv) = refs[17:35]
    frames = refs[35:]
    sends = steps - 2
    trials, block = membrane.shape
    tiles = weights.shape[2]
    rank = lax.axis_index("rank")
    area = lax.axis_index("area")
    sizes, offsets = peer_orders(ranks)

    barrier = pltpu.get_barrier_semaphore()
    for offset in offsets:
        pl.semaphore_signal(barrier, 1, device_id={"rank": peer_of(rank, sizes, offset)}, device_id_type=MESH)
    for near in (-1, 1):
        @pl.when((area + near >= 0) & (area + near < areas))
        def _():
            pl.semaphore_signal(barrier, 1, device_id={"area": (area + near + areas) % areas}, device_id_type=MESH)
    neighbours = (area + areas - 1) // areas + (2 * areas - 2 - area) // areas

    loads = [
        (membrane, v_in), (trace, s_in), (pending, pend), (inter, inter_v), (ext, ext_v),
        (decay, decay_v), (trace_decay, td_v), (threshold, th_v), (tile_source, src_s),
        (amp.at[0, 0], got_amp.at[area]), (target.at[0, 0], got_target.at[area]),
        (count.at[0, 0], got_count.at[area]),
    ] + [(weights.at[0, 0, k], w_v.at[pl.ds(k * block, block)]) for k in range(tiles)]
    copies = [pltpu.make_async_copy(a, b, load_sem.at[n]) for n, (a, b) in enumerate(loads)]
    for copy in copies:
        copy.start()
    for copy in copies[:8]:
        copy.wait()

    shape = (trials, block)
    m_decay = jnp.broadcast_to(decay_v[...], shape)
    t_decay = jnp.broadcast_to(td_v[...], shape)
    twice_limit = jnp.broadcast_to(2.0 * th_v[...], shape)

    def advance(t, v, s, current):
        kept = m_decay * v + (inter_v[t] + 0.25 * ext_v[t].astype(jnp.float32))
        faded = t_decay * s + 0.5
        v = kept + current
        bend = jnp.tanh(2.0 * v - twice_limit)
        return v * (0.5 - 0.5 * bend), faded + 0.5 * bend

    def send(t, s):
        frames[t][rank] = s.astype(jnp.bfloat16)
        if t == 0:
            pl.semaphore_wait(barrier, ranks - 1 + neighbours)
        started = []
        for offset in offsets:
            started.append(pltpu.make_async_remote_copy(
                src_ref=frames[t].at[rank], dst_ref=frames[t].at[rank],
                send_sem=send_sem.at[t], recv_sem=recv_sem.at[t],
                device_id={"rank": peer_of(rank, sizes, offset)}, device_id_type=MESH))
        for copy in started:
            copy.start()

    def all_of(t, sem):
        part = frames[t].at[pl.ds(0, ranks - 1)]
        return pltpu.make_async_copy(part, part, sem.at[t])

    v, s = advance(0, v_in[...], s_in[...], pend[0])
    send(0, s)
    v, s = advance(1, v, s, pend[1])
    send(1, s)
    for copy in copies[8:]:
        copy.wait()
    source = [src_s[0, 0, k] for k in range(tiles)]

    def passing(owner, near):
        other = (area + near + areas) % areas
        return [pltpu.make_async_remote_copy(
            src_ref=box.at[owner], dst_ref=box.at[owner], send_sem=list_send.at[owner, (1 - near) // 2, n],
            recv_sem=list_recv.at[owner, n], device_id={"area": other}, device_id_type=MESH)
            for n, box in enumerate((got_amp, got_target, got_count))]

    def hop(distance, act):
        for near in (-1, 1):
            owner = area - near * (distance - 1)
            inside = (owner >= 0) & (owner < areas) & (area + near >= 0) & (area + near < areas)

            @pl.when(inside)
            def _():
                for copy in passing((owner + areas) % areas, near):
                    act(copy)

    def arrived(distance):
        for near in (-1, 1):
            owner = area - near * distance

            @pl.when((owner >= 0) & (owner < areas))
            def _():
                for copy in passing((owner + areas) % areas, near):
                    copy.wait_recv()

    def exchange(distance):
        if distance > 1:
            arrived(distance - 1)
        hop(distance, lambda copy: copy.start())

    def deliver():
        width = got_amp.shape[3]
        lanes = 128
        groups = block // lanes
        rows = groups * steps * trials
        eye = lax.broadcasted_iota(jnp.int32, (trials, trials), 0) == lax.broadcasted_iota(
            jnp.int32, (trials, trials), 1)
        mine = lax.broadcasted_iota(jnp.int32, (areas, trials), 0) == area
        slot = lax.broadcasted_iota(jnp.int32, (trials, width), 1)
        trial = lax.broadcasted_iota(jnp.int32, (trials, width), 0)
        row_id = lax.broadcasted_iota(jnp.int32, (rows, width), 0)
        lane_id = lax.broadcasted_iota(jnp.int32, (lanes, width), 0)
        total = None
        for a in range(areas):
            live = jnp.sum(jnp.where(mine, got_count[a].astype(jnp.float32), 0.0), axis=0, keepdims=True)
            live = jnp.sum(jnp.where(eye, jnp.broadcast_to(live, (trials, trials)), 0.0), axis=1, keepdims=True)
            value = jnp.where(slot < live.astype(jnp.int32), got_amp[a, area].astype(jnp.float32), 0.0)
            g = got_target[a, area]
            cell = g % block
            key = (cell // lanes) * (steps * trials) + (g // block) * trials + trial
            low = cell % lanes
            left, right = [], []
            for i in range(trials):
                left.append(jnp.where(row_id == key[i:i + 1], value[i:i + 1], 0.0).astype(jnp.bfloat16))
                right.append(jnp.where(lane_id == low[i:i + 1], 1.0, 0.0).astype(jnp.bfloat16))
            part = lax.dot_general(
                jnp.concatenate(left, axis=1), jnp.concatenate(right, axis=1), (((1,), (1,)), ((), ())),
                preferred_element_type=jnp.float32)
            total = part if total is None else total + part
        for c in range(groups):
            for d in range(steps):
                r = (c * steps + d) * trials
                delivered_out[d, :, c * lanes:(c + 1) * lanes] = total[r:r + trials]

    exchange(1)
    for t in range(2, steps):
        all_of(t - 2, recv_sem).wait()
        chosen = jnp.concatenate([frames[t - 2][src] for src in source], axis=1)
        current = jnp.dot(chosen, w_v[...], preferred_element_type=jnp.float32)
        v, s = advance(t, v, s, current)
        if t < sends:
            send(t, s)
        else:
            late_out[t - sends] = s.astype(jnp.bfloat16)
        if t < steps - 3 and t < areas:
            exchange(t)
        if t == steps - 4:
            for distance in range(steps - 3, areas):
                exchange(distance)
            arrived(areas - 1)
            deliver()
    voltage_out[...] = v
    trace_out[...] = s
    for t in range(sends):
        all_of(t, send_sem).wait()
    for distance in range(1, areas):
        hop(distance, lambda copy: copy.wait_send())


def hand_over(*refs):
    sems = refs[8]
    copies = [pltpu.make_async_copy(refs[n], refs[4 + n], sems.at[n]) for n in range(4)]
    for copy in copies:
        copy.start()
    for copy in copies:
        copy.wait()


def on_device(areas, ranks, *args):
    (membrane, synaptic_trace, pending, inter_input, ext_spikes, mem_decay, trace_decay_factor, threshold,
     weight_tiles, tile_source, send_amp, send_target, send_count) = args
    trials, block = membrane.shape
    steps = inter_input.shape[0]
    tiles = weight_tiles.shape[2]
    width = send_amp.shape[4]
    f32, i32, bf16 = jnp.float32, jnp.int32, jnp.bfloat16
    vmem = pltpu.VMEM
    dma = pltpu.SemaphoreType.DMA
    shapes = (
        jax.ShapeDtypeStruct((trials, block), f32),
        jax.ShapeDtypeStruct((trials, block), f32),
        jax.ShapeDtypeStruct((2, trials, block), bf16),
        jax.ShapeDtypeStruct((steps, trials, block), f32),
    )
    results = pl.pallas_call(
        functools.partial(kernel, areas, ranks, steps),
        out_shape=tuple(vmem(x.shape, x.dtype) for x in shapes),
        in_specs=[pl.BlockSpec(memory_space=pltpu.HBM)] * 13,
        out_specs=(pl.BlockSpec(memory_space=pltpu.VMEM),) * 4,
        scratch_shapes=[
            vmem((trials, block), f32), vmem((trials, block), f32), vmem((2, trials, block), f32),
            vmem((steps, trials, block), f32), vmem((steps, trials, block), i32),
            vmem((1, block), f32), vmem((1, block), f32), vmem((1, block), f32),
            vmem((tiles * block, block), bf16), pltpu.SMEM((1, 1, tiles), i32),
            vmem((areas, areas, trials, width), bf16), vmem((areas, areas, trials, width), i32),
            vmem((areas, areas, trials), i32),
            dma((12 + tiles,)), dma((steps - 2,)), dma((steps - 2,)),
            dma((areas, 2, 3)), dma((areas, 3)),
        ] + [vmem((ranks, trials, block), bf16) for _ in range(steps - 2)],
        compiler_params=pltpu.CompilerParams(collective_id=0, has_side_effects=True),
    )(membrane, synaptic_trace, pending, inter_input, ext_spikes, mem_decay.reshape(1, block),
      trace_decay_factor.reshape(1, block), threshold.reshape(1, block), weight_tiles, tile_source,
      send_amp, send_target, send_count)
    return pl.pallas_call(
        hand_over,
        out_shape=shapes,
        in_specs=[pl.BlockSpec(memory_space=pl.ANY)] * 4,
        out_specs=(pl.BlockSpec(memory_space=pltpu.HBM),) * 4,
        scratch_shapes=[dma((4,))],
        compiler_params=pltpu.CompilerParams(vmem_limit_bytes=1 << 20),
    )(*results)


def solution(mesh):
    both = ("area", "rank")
    placed = (
        P(None, both), P(None, both), P(None, None, both), P(None, None, both), P(None, None, both),
        P(both), P(both), P(both), P("area", "rank", None, None, None), P("area", "rank", None),
        P("area", "rank", None, None, None), P("area", "rank", None, None, None),
        P("area", "rank", None, None),
    )
    return jax.shard_map(
        functools.partial(on_device, mesh.shape["area"], mesh.shape["rank"]),
        mesh=mesh,
        in_specs=placed,
        out_specs=(P(None, both), P(None, both), P(None, None, both), P(None, None, both)),
        check_vma=False,
    )
```

```python
import functools

import jax
import jax.numpy as jnp
from jax import lax
from jax.experimental import pallas as pl
from jax.experimental.pallas import tpu as pltpu
from jax.sharding import PartitionSpec as P

MESH = pl.DeviceIdType.MESH


def peer_orders(count):
    core = 2 if count % 2 == 0 else 1
    inner = 2 if count % (2 * core) == 0 else 1
    outer = count // (core * inner)
    offsets = [(a, b, c) for a in range(outer) for b in range(inner) for c in range(core)]
    offsets = [o for o in offsets if o != (0, 0, 0)]
    offsets.sort(key=lambda o: -((o[0] != 0) + (o[1] != 0)))
    return (outer, inner, core), offsets


def peer_of(me, sizes, offset):
    outer, inner, core = sizes
    a = (me // (inner * core) + offset[0]) % outer
    b = (me // core % inner + offset[1]) % inner
    c = (me % core + offset[2]) % core if offset[:2] == (0, 0) else offset[2]
    return (a * inner + b) * core + c


def kernel(areas, ranks, steps, *refs):
    (membrane, trace, pending, inter, ext, decay, trace_decay, threshold, weights, tile_source,
     amp, target, count) = refs[:13]
    voltage_out, trace_out, late_out, delivered_out = refs[13:17]
    (v_in, s_in, pend, inter_v, ext_v, decay_v, td_v, th_v, w_v, src_s, got_amp, got_target, got_count,
     load_sem, send_sem, recv_sem, list_send, list_recv) = refs[17:35]
    frames = refs[35:]
    sends = steps - 2
    trials, block = membrane.shape
    tiles = weights.shape[2]
    rank = lax.axis_index("rank")
    area = lax.axis_index("area")
    sizes, offsets = peer_orders(ranks)

    barrier = pltpu.get_barrier_semaphore()
    for offset in offsets:
        pl.semaphore_signal(barrier, 1, device_id={"rank": peer_of(rank, sizes, offset)}, device_id_type=MESH)
    for near in (-1, 1):
        @pl.when((area + near >= 0) & (area + near < areas))
        def _():
            pl.semaphore_signal(barrier, 1, device_id={"area": (area + near + areas) % areas}, device_id_type=MESH)
    neighbours = (area + areas - 1) // areas + (2 * areas - 2 - area) // areas

    loads = [
        (membrane, v_in), (trace, s_in), (pending, pend), (inter, inter_v), (ext, ext_v),
        (decay, decay_v), (trace_decay, td_v), (threshold, th_v), (tile_source, src_s),
        (amp.at[0, 0], got_amp.at[area]), (target.at[0, 0], got_target.at[area]),
        (count.at[0, 0], got_count.at[area]),
    ] + [(weights.at[0, 0, k], w_v.at[pl.ds(k * block, block)]) for k in range(tiles)]
    copies = [pltpu.make_async_copy(a, b, load_sem.at[n]) for n, (a, b) in enumerate(loads)]
    for copy in copies:
        copy.start()
    for copy in copies[:8]:
        copy.wait()

    shape = (trials, block)
    m_decay = jnp.broadcast_to(decay_v[...], shape)
    t_decay = jnp.broadcast_to(td_v[...], shape)
    twice_limit = jnp.broadcast_to(2.0 * th_v[...], shape)

    def advance(t, v, s, current):
        kept = m_decay * v + (inter_v[t] + 0.25 * ext_v[t].astype(jnp.float32))
        faded = t_decay * s + 0.5
        v = kept + current
        bend = jnp.tanh(2.0 * v - twice_limit)
        return v * (0.5 - 0.5 * bend), faded + 0.5 * bend

    def send(t, s):
        frames[t][rank] = s.astype(jnp.bfloat16)
        if t == 0:
            pl.semaphore_wait(barrier, ranks - 1 + neighbours)
        started = []
        for offset in offsets:
            started.append(pltpu.make_async_remote_copy(
                src_ref=frames[t].at[rank], dst_ref=frames[t].at[rank],
                send_sem=send_sem.at[t], recv_sem=recv_sem.at[t],
                device_id={"rank": peer_of(rank, sizes, offset)}, device_id_type=MESH))
        for copy in started:
            copy.start()

    def all_of(t, sem):
        part = frames[t].at[pl.ds(0, ranks - 1)]
        return pltpu.make_async_copy(part, part, sem.at[t])

    v, s = advance(0, v_in[...], s_in[...], pend[0])
    send(0, s)
    v, s = advance(1, v, s, pend[1])
    send(1, s)
    for copy in copies[8:]:
        copy.wait()
    source = [src_s[0, 0, k] for k in range(tiles)]

    def passing(owner, near):
        other = (area + near + areas) % areas
        return [pltpu.make_async_remote_copy(
            src_ref=box.at[owner], dst_ref=box.at[owner], send_sem=list_send.at[owner, (1 - near) // 2, n],
            recv_sem=list_recv.at[owner, n], device_id={"area": other}, device_id_type=MESH)
            for n, box in enumerate((got_amp, got_target, got_count))]

    def hop(distance, act):
        for near in (-1, 1):
            owner = area - near * (distance - 1)
            inside = (owner >= 0) & (owner < areas) & (area + near >= 0) & (area + near < areas)

            @pl.when(inside)
            def _():
                for copy in passing((owner + areas) % areas, near):
                    act(copy)

    def arrived(distance):
        for near in (-1, 1):
            owner = area - near * distance

            @pl.when((owner >= 0) & (owner < areas))
            def _():
                for copy in passing((owner + areas) % areas, near):
                    copy.wait_recv()

    def exchange(distance):
        if distance > 1:
            arrived(distance - 1)
        hop(distance, lambda copy: copy.start())

    def deliver():
        width = got_amp.shape[3]
        lanes = 128
        groups = block // lanes
        rows = groups * steps * trials
        eye = lax.broadcasted_iota(jnp.int32, (trials, trials), 0) == lax.broadcasted_iota(
            jnp.int32, (trials, trials), 1)
        mine = lax.broadcasted_iota(jnp.int32, (areas, trials), 0) == area
        slot = lax.broadcasted_iota(jnp.int32, (trials, width), 1)
        trial = lax.broadcasted_iota(jnp.int32, (trials, width), 0)
        row_id = lax.broadcasted_iota(jnp.int32, (rows, width), 0)
        lane_id = lax.broadcasted_iota(jnp.int32, (lanes, width), 0)
        total = None
        for a in range(areas):
            live = jnp.sum(jnp.where(mine, got_count[a].astype(jnp.float32), 0.0), axis=0, keepdims=True)
            live = jnp.sum(jnp.where(eye, jnp.broadcast_to(live, (trials, trials)), 0.0), axis=1, keepdims=True)
            value = jnp.where(slot < live.astype(jnp.int32), got_amp[a, area].astype(jnp.float32), 0.0)
            g = got_target[a, area]
            cell = g % block
            key = (cell // lanes) * (steps * trials) + (g // block) * trials + trial
            low = cell % lanes
            left, right = [], []
            for i in range(trials):
                left.append(jnp.where(row_id == key[i:i + 1], value[i:i + 1], 0.0).astype(jnp.bfloat16))
                right.append(jnp.where(lane_id == low[i:i + 1], 1.0, 0.0).astype(jnp.bfloat16))
            part = lax.dot_general(
                jnp.concatenate(left, axis=1), jnp.concatenate(right, axis=1), (((1,), (1,)), ((), ())),
                preferred_element_type=jnp.float32)
            total = part if total is None else total + part
        for c in range(groups):
            for d in range(steps):
                r = (c * steps + d) * trials
                delivered_out[d, :, c * lanes:(c + 1) * lanes] = total[r:r + trials]

    exchange(1)
    reached = 2
    for t in range(2, steps):
        all_of(t - 2, recv_sem).wait()
        chosen = jnp.concatenate([frames[t - 2][src] for src in source], axis=1)
        current = jnp.dot(chosen, w_v[...], preferred_element_type=jnp.float32)
        v, s = advance(t, v, s, current)
        if t < sends:
            send(t, s)
        else:
            late_out[t - sends] = s.astype(jnp.bfloat16)
        if t % 2 == 1 and t < steps - 3 and reached < areas:
            exchange(reached)
            reached += 1
        if t == steps - 3:
            for distance in range(reached, areas):
                exchange(distance)
            arrived(areas - 1)
            deliver()
    voltage_out[...] = v
    trace_out[...] = s
    for t in range(sends):
        all_of(t, send_sem).wait()
    for distance in range(1, areas):
        hop(distance, lambda copy: copy.wait_send())


def hand_over(*refs):
    sems = refs[8]
    copies = [pltpu.make_async_copy(refs[n], refs[4 + n], sems.at[n]) for n in range(4)]
    for copy in copies:
        copy.start()
    for copy in copies:
        copy.wait()


def on_device(areas, ranks, *args):
    (membrane, synaptic_trace, pending, inter_input, ext_spikes, mem_decay, trace_decay_factor, threshold,
     weight_tiles, tile_source, send_amp, send_target, send_count) = args
    trials, block = membrane.shape
    steps = inter_input.shape[0]
    tiles = weight_tiles.shape[2]
    width = send_amp.shape[4]
    f32, i32, bf16 = jnp.float32, jnp.int32, jnp.bfloat16
    vmem = pltpu.VMEM
    dma = pltpu.SemaphoreType.DMA
    shapes = (
        jax.ShapeDtypeStruct((trials, block), f32),
        jax.ShapeDtypeStruct((trials, block), f32),
        jax.ShapeDtypeStruct((2, trials, block), bf16),
        jax.ShapeDtypeStruct((steps, trials, block), f32),
    )
    results = pl.pallas_call(
        functools.partial(kernel, areas, ranks, steps),
        out_shape=tuple(vmem(x.shape, x.dtype) for x in shapes),
        in_specs=[pl.BlockSpec(memory_space=pltpu.HBM)] * 13,
        out_specs=(pl.BlockSpec(memory_space=pltpu.VMEM),) * 4,
        scratch_shapes=[
            vmem((trials, block), f32), vmem((trials, block), f32), vmem((2, trials, block), f32),
            vmem((steps, trials, block), f32), vmem((steps, trials, block), i32),
            vmem((1, block), f32), vmem((1, block), f32), vmem((1, block), f32),
            vmem((tiles * block, block), bf16), pltpu.SMEM((1, 1, tiles), i32),
            vmem((areas, areas, trials, width), bf16), vmem((areas, areas, trials, width), i32),
            vmem((areas, areas, trials), i32),
            dma((12 + tiles,)), dma((steps - 2,)), dma((steps - 2,)),
            dma((areas, 2, 3)), dma((areas, 3)),
        ] + [vmem((ranks, trials, block), bf16) for _ in range(steps - 2)],
        compiler_params=pltpu.CompilerParams(collective_id=0, has_side_effects=True),
    )(membrane, synaptic_trace, pending, inter_input, ext_spikes, mem_decay.reshape(1, block),
      trace_decay_factor.reshape(1, block), threshold.reshape(1, block), weight_tiles, tile_source,
      send_amp, send_target, send_count)
    return pl.pallas_call(
        hand_over,
        out_shape=shapes,
        in_specs=[pl.BlockSpec(memory_space=pl.ANY)] * 4,
        out_specs=(pl.BlockSpec(memory_space=pltpu.HBM),) * 4,
        scratch_shapes=[dma((4,))],
        compiler_params=pltpu.CompilerParams(vmem_limit_bytes=1 << 20),
    )(*results)


def solution(mesh):
    both = ("area", "rank")
    placed = (
        P(None, both), P(None, both), P(None, None, both), P(None, None, both), P(None, None, both),
        P(both), P(both), P(both), P("area", "rank", None, None, None), P("area", "rank", None),
        P("area", "rank", None, None, None), P("area", "rank", None, None, None),
        P("area", "rank", None, None),
    )
    return jax.shard_map(
        functools.partial(on_device, mesh.shape["area"], mesh.shape["rank"]),
        mesh=mesh,
        in_specs=placed,
        out_specs=(P(None, both), P(None, both), P(None, None, both), P(None, None, both)),
        check_vma=False,
    )
```
